32 devices in a mesh: grp: 1, win: 32 (over z, y, x, core).
Axes of the slice: x: 2, y: 2, z: 4, core: 2. Of those that a mesh axis runs over, the one named last changes fastest.
Arguments:
- tokens: bfloat16 [2, 8, 64, 96, 384], P('grp', None, None, 'win'), may hold values from -6 to 6
- w_upper: bfloat16 [384, 640], replicated, may hold values from -0.3125 to 0.3125
- w_surface: bfloat16 [384, 256], replicated, may hold values from -0.3125 to 0.3125
- bias: float32 [69], replicated, may hold values from -1 to 1
Outputs:
- fields: bfloat16 [2, 17664, 384], P('grp', 'win')
The draws below stay inside these ranges and needn't reach their ends.
All inputs are finite; a program needn't handle non-finite values.
Results may differ from the reference program's by a relative error of at most 0.0048.
Values may be sent and summed in bfloat16 or wider, within the bound.
A program may use at most 128 MiB of HBM per device.

```python
import jax
import jax.numpy as jnp
from jax import lax

D = 384
VARS_UP = 5
LEVELS = 13
VARS_SF = 4
PATCH = 4
MEMB = 2
LAT_TOK = 64
LON_DEV = 3
LEV_TOK = 8
NLON = 96
OUT_CH = 69
N_WIN = 32


def steps_of(key, dims, split, least, largest):
    level, own = 1.0, jax.random.fold_in(key, 6)
    for dim, parts in split:
        steps = jnp.exp(jax.random.uniform(jax.random.fold_in(own, dim), (parts,), jnp.float32, least / len(split), largest / len(split)))
        level = level * jnp.repeat(steps, dims[dim] // parts).reshape([-1 if axis == dim else 1 for axis in range(len(dims))])
    return level


def normal_values(own_key, extent, scale, most, cuts=(), held_as=jnp.bfloat16):
    entries = scale * jax.random.normal(own_key, extent, jnp.float32)
    if cuts:
        entries = entries * steps_of(own_key, extent, cuts, -0.22, 0.18)
    return jnp.clip(entries, -most, most).astype(held_as)


def setup_inputs(seed: int = 0, part: int = 0) -> dict:
    streams_of = jax.random.split(jax.random.key(seed), 5)
    own_keys = jax.random.split(jax.random.fold_in(streams_of[4], part), 5)
    return {
        "tokens": normal_values(own_keys[0], (MEMB, LEV_TOK, LAT_TOK, NLON, D), 1.0, 6.0, ((3, 32),)),
        "w_upper": normal_values(streams_of[1], (D, VARS_UP * 8 * PATCH * PATCH), D ** -0.5, 0.3125),
        "w_surface": normal_values(streams_of[2], (D, VARS_SF * 4 * PATCH * PATCH), D ** -0.5, 0.3125),
        "bias": jnp.clip(jax.random.uniform(streams_of[3], (OUT_CH,), jnp.float32, -1.0, 1.0), -1.0, 1.0),
    }


def intersection_add(values, axis):
    first = lax.index_in_dim(values, 0, axis + 1, keepdims=False)
    second = lax.index_in_dim(values, 1, axis + 1, keepdims=False)
    pad_first = [(0, 0)] * first.ndim
    pad_second = [(0, 0)] * first.ndim
    pad_first[axis] = (0, 1)
    pad_second[axis] = (1, 0)
    return jnp.pad(first, pad_first) + jnp.pad(second, pad_second)


def project(tokens, w_upper, w_surface):
    members, tok_levels, lat_rows, lon_cols, width = tokens.shape
    upper_levels = tok_levels - 1
    rim_width = PATCH // 2
    upper = jnp.einsum("mzijd,dn->mzijn", tokens[:, :upper_levels], w_upper, preferred_element_type=jnp.float32)
    upper = upper.reshape(members, upper_levels, lat_rows, lon_cols, VARS_UP, 2, 2, PATCH, 2, PATCH)
    upper = jnp.transpose(upper, (0, 4, 1, 5, 2, 6, 7, 3, 8, 9))
    upper = intersection_add(upper, 4)
    upper = intersection_add(upper, 6)
    upper = upper.reshape(members, VARS_UP, 2 * upper_levels, (lat_rows + 1) * PATCH, (lon_cols + 1) * PATCH)
    upper = upper[:, :, :LEVELS, rim_width:rim_width + lat_rows * PATCH]
    upper = upper.reshape(members, VARS_UP * LEVELS, lat_rows * PATCH, (lon_cols + 1) * PATCH)
    surface = jnp.einsum("mijd,dn->mijn", tokens[:, upper_levels], w_surface, preferred_element_type=jnp.float32)
    surface = surface.reshape(members, lat_rows, lon_cols, VARS_SF, 2, PATCH, 2, PATCH)
    surface = jnp.transpose(surface, (0, 3, 1, 4, 5, 2, 6, 7))
    surface = intersection_add(surface, 2)
    surface = intersection_add(surface, 4)
    surface = surface.reshape(members, VARS_SF, (lat_rows + 1) * PATCH, (lon_cols + 1) * PATCH)
    surface = surface[:, :, rim_width:rim_width + lat_rows * PATCH]
    joined = jnp.concatenate([upper, surface], axis=1).astype(jnp.bfloat16)
    return joined.reshape(members, -1, (lon_cols + 1) * PATCH)


def reference(tokens, w_upper, w_surface, bias):
    members = tokens.shape[0]
    lat_rows = tokens.shape[2]
    rim_width = PATCH // 2

    def one_window(window):
        start = (window * LON_DEV).astype(jnp.int32)
        piece = lax.dynamic_slice_in_dim(tokens, start, LON_DEV, 3)
        return project(piece, w_upper, w_surface)

    frames = lax.map(one_window, jnp.arange(N_WIN, dtype=jnp.int32))
    frame_width = frames.shape[3]
    inner = frames[:, :, :, rim_width:frame_width - rim_width].astype(jnp.float32)
    columns = inner.shape[3]
    from_left = jnp.roll(frames[:, :, :, frame_width - rim_width:], 1, axis=0).astype(jnp.float32)
    from_right = jnp.roll(frames[:, :, :, :rim_width], -1, axis=0).astype(jnp.float32)
    edges = ((0, 0), (0, 0), (0, 0))
    summed = inner + jnp.pad(from_left, edges + ((0, columns - rim_width),))
    summed = summed + jnp.pad(from_right, edges + ((columns - rim_width, 0),))
    bias_rows = jnp.repeat(bias, lat_rows * PATCH)
    image = (summed + bias_rows[None, None, :, None]).astype(jnp.bfloat16)
    image = jnp.transpose(image, (1, 2, 0, 3))
    return image.reshape(members, image.shape[1], N_WIN * columns)
```

```python
import functools

import jax
import jax.numpy as jnp
from jax import lax
from jax.experimental import pallas as pl
from jax.experimental.pallas import tpu as pltpu
from jax.sharding import PartitionSpec as P

VARS_UP = 5
LEVELS = 13
VARS_SF = 4
PATCH = 4
GROUP = 8
CHANNELS = VARS_UP * LEVELS + VARS_SF


def spans_of(owners, own_rows):
    return [
        (o * own_rows // PATCH, -(-(o + 1) * own_rows // PATCH)) for o in range(owners)
    ]


def selector(second, column):
    row = lax.broadcasted_iota(jnp.int32, (128, 128), 0)
    n = lax.broadcasted_iota(jnp.int32, (128, 128), 1)
    step = (n // 16) % 4 - column
    source = (n // 64) * 64 + (((n // 4) % 4 + 2 + 4 * second) % 8) * 8 + n % 4 + 4 * step
    hit = (row == source) & (step >= 0) & (step <= 1)
    return jnp.where(hit, 1.0, 0.0).astype(jnp.bfloat16)


def send_kernel(spans, pad_rows, tok_ref, wu_ref, ws_ref, wire_ref, wb_ref, y_ref, frame_ref):
    members, tok_levels, lon_cols, lat_rows, width = tok_ref.shape
    upper_levels = tok_levels - 1
    up_tiles = wu_ref.shape[1] // 128
    sf_tiles = ws_ref.shape[1] // 128
    sel = jnp.concatenate(
        [selector(y, j) for j in range(lon_cols) for y in range(2)], axis=1
    )
    for t in range(up_tiles + sf_tiles):
        if t < up_tiles:
            w = wu_ref[:, t * 128 : (t + 1) * 128]
        else:
            w = ws_ref[:, (t - up_tiles) * 128 : (t - up_tiles + 1) * 128]
        spread = jnp.dot(w, sel, preferred_element_type=jnp.float32).astype(jnp.bfloat16)
        for j in range(lon_cols):
            wb_ref[t, j * width : (j + 1) * width, :] = spread[:, j * 256 : (j + 1) * 256]
    lane = lax.broadcasted_iota(jnp.int32, (lat_rows, 128), 1)
    line = lax.broadcasted_iota(jnp.int32, (lat_rows, 128), 0)
    lower = (lane // 4) % 4 < 2
    low_lanes = lane < 64
    edge = jnp.where(lower, 0, lat_rows - 1)
    keep = line != edge

    def image(y):
        first, second = y[:, :128], y[:, 128:]
        moved = jnp.where(
            lower, pltpu.roll(second, 1, 0), pltpu.roll(second, lat_rows - 1, 0)
        )
        return first + jnp.where(keep, moved, 0.0)

    def put(channel, block):
        base = channel * lat_rows
        for o, (lo, hi) in enumerate(spans):
            a, b = max(lo, base), min(hi, base + lat_rows)
            if a < b:
                frame_ref[o, a - lo : b - lo, :] = block[a - base : b - base]

    def merge(even_channel, odd_channel, one, two):
        put(even_channel, jnp.where(low_lanes, one, pltpu.roll(two, 64, 1)))
        if odd_channel is not None:
            put(odd_channel, jnp.where(low_lanes, pltpu.roll(one, 64, 1), two))

    for t in range(up_tiles + sf_tiles):
        if t < up_tiles:
            levels = list(range(upper_levels))
        else:
            levels = [upper_levels]
        for m in range(members):
            z0, z1 = levels[0], levels[-1] + 1
            rows = (z1 - z0) * lat_rows
            total = None
            for j in range(lon_cols):
                part = jnp.dot(
                    tok_ref[m, z0:z1, j].reshape(rows, width),
                    wb_ref[t, j * width : (j + 1) * width, :],
                    preferred_element_type=jnp.float32,
                )
                total = part if total is None else total + part
            y_ref[m, :rows] = total
        for i, z in enumerate(levels):
            one, two = (
                image(y_ref[m, i * lat_rows : (i + 1) * lat_rows, :]) for m in range(members)
            )
            if t < up_tiles:
                even = t * LEVELS + 2 * z
                odd = even + 1 if 2 * z + 1 < LEVELS else None
            else:
                even = VARS_UP * LEVELS + 2 * (t - up_tiles)
                odd = even + 1
            merge(even, odd, one, two)
    wire_ref[...] = frame_ref[...].astype(jnp.bfloat16)


def compose(lat_rows, own_rows, got_ref, place_ref, bias_ref, out_ref, y_ref, image_ref):
    windows, pad_rows, _ = got_ref.shape
    members, _, lons = out_ref.shape
    groups = windows // GROUP
    tiles = lons // 128
    pitch = lons // groups
    for g in range(groups):
        stacked = jnp.concatenate([got_ref[g * GROUP + i] for i in range(GROUP)], axis=1)
        y_ref[g] = jnp.dot(stacked, place_ref[...], preferred_element_type=jnp.float32)
    lane = lax.broadcasted_iota(jnp.int32, (pad_rows, 128), 1)
    for m in range(members):
        for q in range(PATCH):
            sums = [None] * tiles
            at = (m * PATCH + q) * 128

            def add(tile, value):
                tile = tile % tiles
                sums[tile] = value if sums[tile] is None else sums[tile] + value

            for g in range(groups):
                start = g * pitch - PATCH // 2
                shift = start % 128
                value = y_ref[g, :, at : at + 128]
                if shift:
                    value = pltpu.roll(value, shift, 1)
                if shift + pitch + PATCH <= 128:
                    add(start // 128, value)
                else:
                    add(start // 128, jnp.where(lane >= shift, value, 0.0))
                    add(start // 128 + 1, jnp.where(lane < shift, value, 0.0))
            for tile in range(tiles):
                image_ref[m, tile, pl.ds(q, pad_rows, stride=PATCH), :] = sums[tile]
    first_row = lax.axis_index("win") * own_rows
    height = lat_rows * PATCH
    row = first_row + lax.broadcasted_iota(jnp.int32, (own_rows, 128), 0)
    first = first_row // height
    last = bias_ref.shape[0] - 1
    offsets = jnp.zeros((own_rows, 128), jnp.float32)
    for i in range((own_rows - 1) // height + 2):
        channel = jnp.minimum(first + i, last)
        begins = (first + i) * height
        offsets = jnp.where(row >= begins, bias_ref[channel], offsets)
    begin = 0 if own_rows % PATCH == 0 else first_row % PATCH
    for m in range(members):
        for tile in range(tiles):
            rows = image_ref[m, tile, pl.ds(begin, own_rows), :]
            out_ref[m, :, tile * 128 : (tile + 1) * 128] = (rows + offsets).astype(jnp.bfloat16)


def placing(members, pitch):
    size = GROUP * 128
    row = lax.broadcasted_iota(jnp.int32, (size, size), 0)
    col = lax.broadcasted_iota(jnp.int32, (size, size), 1)
    target = (row // 64) % 2 * 512 + (row // 4) % 4 * 128
    target = target + row // 128 * pitch + (row // 16) % 4 * 4 + row % 4
    return (target == col).astype(jnp.bfloat16)


def body(tokens, w_upper, w_surface, bias):
    members, tok_levels, lat_rows, lon_cols, width = tokens.shape
    windows = lax.axis_size("win")
    own_rows = CHANNELS * lat_rows * PATCH // windows
    lons = windows * lon_cols * PATCH
    spans = spans_of(windows, own_rows)
    pad_rows = -(-max(hi - lo for lo, hi in spans) // 16) * 16
    tiles = w_upper.shape[1] // 128 + w_surface.shape[1] // 128
    wire = pl.pallas_call(
        functools.partial(send_kernel, spans, pad_rows),
        out_shape=jax.ShapeDtypeStruct((windows, pad_rows, 128), jnp.bfloat16),
        in_specs=[pl.BlockSpec(memory_space=pltpu.VMEM)] * 3,
        out_specs=pl.BlockSpec(memory_space=pltpu.VMEM),
        scratch_shapes=[
            pltpu.VMEM((tiles, lon_cols * width, 256), jnp.bfloat16),
            pltpu.VMEM((members, (tok_levels - 1) * lat_rows, 256), jnp.float32),
            pltpu.VMEM((windows, pad_rows, 128), jnp.float32),
        ],
        compiler_params=pltpu.CompilerParams(vmem_limit_bytes=32 * 1024 * 1024),
    )(jnp.transpose(tokens, (0, 1, 3, 2, 4)), w_upper, w_surface)
    got = lax.all_to_all(wire, "win", split_axis=0, concat_axis=0, tiled=True)
    place = placing(members, lon_cols * PATCH)
    return pl.pallas_call(
        functools.partial(compose, lat_rows, own_rows),
        out_shape=jax.ShapeDtypeStruct((members, own_rows, lons), jnp.bfloat16),
        in_specs=[
            pl.BlockSpec(memory_space=pltpu.VMEM),
            pl.BlockSpec(memory_space=pltpu.VMEM),
            pl.BlockSpec(memory_space=pltpu.SMEM),
        ],
        out_specs=pl.BlockSpec(memory_space=pltpu.VMEM),
        scratch_shapes=[
            pltpu.VMEM((windows // GROUP, pad_rows, GROUP * 128), jnp.float32),
            pltpu.VMEM((members, lons // 128, pad_rows * PATCH, 128), jnp.float32),
        ],
        compiler_params=pltpu.CompilerParams(vmem_limit_bytes=32 * 1024 * 1024),
    )(got, place, bias)


def solution(mesh):
    placed = (P("grp", None, None, "win", None), P(), P(), P())
    return jax.shard_map(
        body, mesh=mesh, in_specs=placed, out_specs=P("grp", "win", None), check_vma=False
    )
```

```python
import functools

import jax
import jax.numpy as jnp
from jax import lax
from jax.experimental import pallas as pl
from jax.experimental.pallas import tpu as pltpu
from jax.sharding import PartitionSpec as P

VARS_UP = 5
LEVELS = 13
VARS_SF = 4
PATCH = 4
GROUP = 8
CHANNELS = VARS_UP * LEVELS + VARS_SF


def spans_of(owners, own_rows):
    return [
        (o * own_rows // PATCH, -(-(o + 1) * own_rows // PATCH)) for o in range(owners)
    ]


def selector(second, column):
    row = lax.broadcasted_iota(jnp.int32, (128, 128), 0)
    n = lax.broadcasted_iota(jnp.int32, (128, 128), 1)
    step = (n // 16) % 4 - column
    source = (n // 64) * 64 + (((n // 4) % 4 + 2 + 4 * second) % 8) * 8 + n % 4 + 4 * step
    hit = (row == source) & (step >= 0) & (step <= 1)
    return jnp.where(hit, 1.0, 0.0).astype(jnp.bfloat16)


def partner(me, r, windows):
    if windows & (windows - 1):
        return lax.rem(me + r, windows)
    return me ^ r


def kernel(
    own_rows, tok_hbm, wu_hbm, ws_hbm, bias_ref, out_ref,
    tok_ref, wu_ref, ws_ref, wb_ref, proj_ref, frame_ref, wire_ref, got_ref, place_ref,
    y_ref, image_ref, load_sem, send_sem, recv_sem,
):
    members, tok_levels, lon_cols, lat_rows, width = tok_ref.shape
    windows, pad_rows, _ = wire_ref.shape
    upper_levels = tok_levels - 1
    up_tiles = wu_ref.shape[1] // 128
    sf_tiles = ws_ref.shape[1] // 128
    me = lax.axis_index("win")

    loads = [
        pltpu.make_async_copy(wu_hbm, wu_ref, load_sem.at[0]),
        pltpu.make_async_copy(ws_hbm, ws_ref, load_sem.at[1]),
        pltpu.make_async_copy(tok_hbm, tok_ref, load_sem.at[2]),
    ]
    for load in loads:
        load.start()

    barrier = pltpu.get_barrier_semaphore()

    def greet(r, carry):
        pl.semaphore_signal(
            barrier, inc=1, device_id={"win": partner(me, r, windows)},
            device_id_type=pl.DeviceIdType.MESH,
        )
        return carry

    lax.fori_loop(1, windows, greet, 0)

    sel = jnp.concatenate(
        [selector(y, j) for j in range(lon_cols) for y in range(2)], axis=1
    )
    loads[0].wait()
    loads[1].wait()
    for t in range(up_tiles + sf_tiles):
        if t < up_tiles:
            w = wu_ref[:, t * 128 : (t + 1) * 128]
        else:
            w = ws_ref[:, (t - up_tiles) * 128 : (t - up_tiles + 1) * 128]
        spread = jnp.dot(w, sel, preferred_element_type=jnp.float32).astype(jnp.bfloat16)
        for j in range(lon_cols):
            wb_ref[t, j * width : (j + 1) * width, :] = spread[:, j * 256 : (j + 1) * 256]
    lane = lax.broadcasted_iota(jnp.int32, (lat_rows, 128), 1)
    line = lax.broadcasted_iota(jnp.int32, (lat_rows, 128), 0)
    lower = (lane // 4) % 4 < 2
    low_lanes = lane < 64
    keep = line != jnp.where(lower, 0, lat_rows - 1)

    def image(y):
        first, second = y[:, :128], y[:, 128:]
        moved = jnp.where(
            lower, pltpu.roll(second, 1, 0), pltpu.roll(second, lat_rows - 1, 0)
        )
        return first + jnp.where(keep, moved, 0.0)

    def put(channel, block):
        start = pl.multiple_of(channel * lat_rows, 8)
        frame_ref[pl.ds(start, lat_rows), :] = block

    def multiply(tile, z0, z1):
        rows = (z1 - z0) * lat_rows
        for m in range(members):
            total = None
            for j in range(lon_cols):
                part = jnp.dot(
                    tok_ref[m, z0:z1, j].reshape(rows, width),
                    wb_ref[tile, j * width : (j + 1) * width, :],
                    preferred_element_type=jnp.float32,
                )
                total = part if total is None else total + part
            proj_ref[m, :rows] = total

    def merge(even_channel, odd_channel, i):
        one, two = (
            image(proj_ref[m, i * lat_rows : (i + 1) * lat_rows, :]) for m in range(members)
        )
        put(even_channel, jnp.where(low_lanes, one, pltpu.roll(two, 64, 1)))
        if odd_channel is not None:
            put(odd_channel, jnp.where(low_lanes, pltpu.roll(one, 64, 1), two))

    def copy_to(r):
        other = partner(me, r, windows)
        return pltpu.make_async_remote_copy(
            src_ref=wire_ref.at[other],
            dst_ref=got_ref.at[me],
            send_sem=send_sem.at[other],
            recv_sem=recv_sem.at[me],
            device_id={"win": other},
            device_id_type=pl.DeviceIdType.MESH,
        )

    def block_of(other):
        start = other * own_rows // PATCH
        return frame_ref[pl.ds(start, pad_rows), :].astype(jnp.bfloat16)

    def pack(r, carry):
        other = partner(me, r, windows)
        wire_ref[other] = block_of(other)
        return carry

    def send(r, carry):
        copy_to(r).start()
        return carry

    tail = CHANNELS * lat_rows
    frame_ref[tail:, :] = jnp.zeros((frame_ref.shape[0] - tail, 128), jnp.float32)
    loads[2].wait()
    for t in range(sf_tiles):
        multiply(up_tiles + t, upper_levels, tok_levels)
        even = VARS_UP * LEVELS + 2 * t
        merge(even, even + 1, 0)
    early = up_tiles // 2 + 1
    turn = jnp.where(me < windows // 2, up_tiles - early, 0)
    half = windows // 2
    for slot in range(up_tiles):
        t = lax.rem(slot + turn, up_tiles)
        multiply(t, 0, upper_levels)
        for z in range(upper_levels):
            even = t * LEVELS + 2 * z
            merge(even, even + 1 if 2 * z + 1 < LEVELS else None, z)
        if slot == early - 1:
            lax.fori_loop(half, windows, pack, 0)
            pl.semaphore_wait(barrier, windows - 1)
            lax.fori_loop(half, windows, send, 0)
    lax.fori_loop(1, half, pack, 0)
    lax.fori_loop(1, half, send, 0)
    got_ref[me] = block_of(me)

    lons = out_ref.shape[2]
    groups = windows // GROUP
    pitch = lons // windows
    row = lax.broadcasted_iota(jnp.int32, (128, GROUP * 128), 0)
    col = lax.broadcasted_iota(jnp.int32, (128, GROUP * 128), 1)
    target = row // 64 * 512 + (row // 4) % 4 * 128 + (row // 16) % 4 * 4 + row % 4

    def fill(i, carry):
        hit = col == target + i * pitch
        place_ref[pl.ds(pl.multiple_of(i * 128, 128), 128), :] = jnp.where(
            hit, 1.0, 0.0
        ).astype(jnp.bfloat16)
        return carry

    lax.fori_loop(0, GROUP, fill, 0)

    def arrived(source):
        pltpu.make_async_remote_copy(
            src_ref=wire_ref.at[source],
            dst_ref=got_ref.at[source],
            send_sem=send_sem.at[source],
            recv_sem=recv_sem.at[source],
            device_id={"win": source},
            device_id_type=pl.DeviceIdType.MESH,
        ).wait_recv()

    def gather(k, carry):
        g = partner(me // GROUP, k, groups)

        def wait_one(i, inner):
            source = g * GROUP + i

            @pl.when(source != me)
            def _():
                arrived(source)

            return inner

        lax.fori_loop(0, GROUP, wait_one, 0)
        stacked = jnp.concatenate([got_ref[g * GROUP + i] for i in range(GROUP)], axis=1)
        y_ref[g] = jnp.dot(stacked, place_ref[...], preferred_element_type=jnp.float32)
        return carry

    lax.fori_loop(0, groups, gather, 0)
    compose(lat_rows, own_rows, me, bias_ref, out_ref, y_ref, image_ref)

    def sent(r, carry):
        copy_to(r).wait_send()
        return carry

    lax.fori_loop(1, windows, sent, 0)


def compose(lat_rows, own_rows, me, bias_ref, out_ref, y_ref, image_ref):
    groups, pad_rows, _ = y_ref.shape
    members, _, lons = out_ref.shape
    tiles = lons // 128
    pitch = lons // groups
    lane = lax.broadcasted_iota(jnp.int32, (pad_rows, 128), 1)
    for m in range(members):
        for q in range(PATCH):
            sums = [None] * tiles
            at = (m * PATCH + q) * 128

            def add(tile, value):
                tile = tile % tiles
                sums[tile] = value if sums[tile] is None else sums[tile] + value

            for g in range(groups):
                start = g * pitch - PATCH // 2
                shift = start % 128
                value = y_ref[g, :, at : at + 128]
                if shift:
                    value = pltpu.roll(value, shift, 1)
                if shift + pitch + PATCH <= 128:
                    add(start // 128, value)
                else:
                    add(start // 128, jnp.where(lane >= shift, value, 0.0))
                    add(start // 128 + 1, jnp.where(lane < shift, value, 0.0))
            for tile in range(tiles):
                image_ref[m, tile, pl.ds(q, pad_rows, stride=PATCH), :] = sums[tile]
    first_row = me * own_rows
    height = lat_rows * PATCH
    row = first_row + lax.broadcasted_iota(jnp.int32, (own_rows, 128), 0)
    first = first_row // height
    last = bias_ref.shape[0] - 1
    offsets = jnp.zeros((own_rows, 128), jnp.float32)
    for i in range((own_rows - 1) // height + 2):
        channel = jnp.minimum(first + i, last)
        begins = (first + i) * height
        offsets = jnp.where(row >= begins, bias_ref[channel], offsets)
    begin = 0 if own_rows % PATCH == 0 else first_row % PATCH
    for m in range(members):
        for tile in range(tiles):
            rows = image_ref[m, tile, pl.ds(begin, own_rows), :]
            out_ref[m, :, tile * 128 : (tile + 1) * 128] = (rows + offsets).astype(jnp.bfloat16)


def body(tokens, w_upper, w_surface, bias):
    members, tok_levels, lat_rows, lon_cols, width = tokens.shape
    windows = lax.axis_size("win")
    own_rows = CHANNELS * lat_rows * PATCH // windows
    lons = windows * lon_cols * PATCH
    spans = spans_of(windows, own_rows)
    pad_rows = -(-max(hi - lo for lo, hi in spans) // 16) * 16
    frame_rows = -(-(spans[-1][0] + pad_rows) // 8) * 8
    tiles = w_upper.shape[1] // 128 + w_surface.shape[1] // 128
    groups = windows // GROUP
    bf16, f32 = jnp.bfloat16, jnp.float32
    by_lon = jnp.transpose(tokens, (0, 1, 3, 2, 4))
    return pl.pallas_call(
        functools.partial(kernel, own_rows),
        out_shape=jax.ShapeDtypeStruct((members, own_rows, lons), bf16),
        in_specs=[pl.BlockSpec(memory_space=pltpu.HBM)] * 3
        + [pl.BlockSpec(memory_space=pltpu.SMEM)],
        out_specs=pl.BlockSpec(memory_space=pltpu.VMEM),
        scratch_shapes=[
            pltpu.VMEM(by_lon.shape, bf16),
            pltpu.VMEM(w_upper.shape, bf16),
            pltpu.VMEM(w_surface.shape, bf16),
            pltpu.VMEM((tiles, lon_cols * width, 256), bf16),
            pltpu.VMEM((members, (tok_levels - 1) * lat_rows, 256), f32),
            pltpu.VMEM((frame_rows, 128), f32),
            pltpu.VMEM((windows, pad_rows, 128), bf16),
            pltpu.VMEM((windows, pad_rows, 128), bf16),
            pltpu.VMEM((GROUP * 128, GROUP * 128), bf16),
            pltpu.VMEM((groups, pad_rows, GROUP * 128), f32),
            pltpu.VMEM((members, lons // 128, pad_rows * PATCH, 128), f32),
            pltpu.SemaphoreType.DMA((3,)),
            pltpu.SemaphoreType.DMA((windows,)),
            pltpu.SemaphoreType.DMA((windows,)),
        ],
        compiler_params=pltpu.CompilerParams(
            collective_id=0, has_side_effects=True, vmem_limit_bytes=65 * 1000 * 1000
        ),
    )(by_lon, w_upper, w_surface, bias)


def solution(mesh):
    placed = (P("grp", None, None, "win", None), P(), P(), P())
    return jax.shard_map(
        body, mesh=mesh, in_specs=placed, out_specs=P("grp", "win", None), check_vma=False
    )
```

```python
import functools

import jax
import jax.numpy as jnp
from jax import lax
from jax.experimental import pallas as pl
from jax.experimental.pallas import tpu as pltpu
from jax.sharding import PartitionSpec as P

VARS_UP = 5
LEVELS = 13
VARS_SF = 4
PATCH = 4
GROUP = 8
CHANNELS = VARS_UP * LEVELS + VARS_SF


def spans_of(owners, own_rows):
    return [
        (o * own_rows // PATCH, -(-(o + 1) * own_rows // PATCH)) for o in range(owners)
    ]


def selector(second, column):
    row = lax.broadcasted_iota(jnp.int32, (128, 128), 0)
    n = lax.broadcasted_iota(jnp.int32, (128, 128), 1)
    step = (n // 16) % 4 - column
    source = (n // 64) * 64 + (((n // 4) % 4 + 2 + 4 * second) % 8) * 8 + n % 4 + 4 * step
    hit = (row == source) & (step >= 0) & (step <= 1)
    return jnp.where(hit, 1.0, 0.0).astype(jnp.bfloat16)


def partner(me, r, windows):
    if windows & (windows - 1):
        return lax.rem(me + r, windows)
    return me ^ r


def kernel(
    plan, tok_hbm, wu_hbm, ws_hbm, bias_ref, out_ref,
    tok_ref, wu_ref, ws_ref, wb_ref, proj_ref, frame_ref, wire_ref, got_ref, place_ref, image_ref,
    load_sem, send_sem, recv_sem,
):
    members, tok_levels, lon_cols, lat_rows, width = tok_ref.shape
    windows, pad_rows, _ = wire_ref.shape
    upper_levels = tok_levels - 1
    up_tiles = wu_ref.shape[1] // 128
    sf_tiles = ws_ref.shape[1] // 128
    me = lax.axis_index("win")

    loads = [
        pltpu.make_async_copy(wu_hbm, wu_ref, load_sem.at[0]),
        pltpu.make_async_copy(ws_hbm, ws_ref, load_sem.at[1]),
        pltpu.make_async_copy(tok_hbm, tok_ref, load_sem.at[2]),
    ]
    for load in loads:
        load.start()

    barrier = pltpu.get_barrier_semaphore()

    def greet(r, carry):
        pl.semaphore_signal(
            barrier, inc=1, device_id={"win": partner(me, r, windows)},
            device_id_type=pl.DeviceIdType.MESH,
        )
        return carry

    lax.fori_loop(1, windows, greet, 0)

    own_rows, low_plan, high_plan = plan
    sel = jnp.concatenate(
        [selector(y, j) for j in range(lon_cols) for y in range(2)], axis=1
    )

    def spread(w):
        wide = jnp.dot(w, sel, preferred_element_type=jnp.float32).astype(jnp.bfloat16)
        for j in range(lon_cols):
            wb_ref[j * width : (j + 1) * width, :] = wide[:, j * 256 : (j + 1) * 256]

    lane = lax.broadcasted_iota(jnp.int32, (lat_rows, 128), 1)
    line = lax.broadcasted_iota(jnp.int32, (lat_rows, 128), 0)
    lower = (lane // 4) % 4 < 2
    low_lanes = lane < 64
    keep = line != jnp.where(lower, 0, lat_rows - 1)

    def image(y):
        first, second = y[:, :128], y[:, 128:]
        moved = jnp.where(
            lower, pltpu.roll(second, 1, 0), pltpu.roll(second, lat_rows - 1, 0)
        )
        return first + jnp.where(keep, moved, 0.0)

    def put(channel, block):
        start = pl.multiple_of(channel * lat_rows, 8)
        frame_ref[pl.ds(start, lat_rows), :] = block

    def multiply(z0, z1):
        rows = (z1 - z0) * lat_rows
        for m in range(members):
            total = None
            for j in range(lon_cols):
                part = jnp.dot(
                    tok_ref[m, z0:z1, j].reshape(rows, width),
                    wb_ref[j * width : (j + 1) * width, :],
                    preferred_element_type=jnp.float32,
                )
                total = part if total is None else total + part
            proj_ref[m, :rows] = total

    def merge(even_channel, odd_channel, i):
        one, two = (
            image(proj_ref[m, i * lat_rows : (i + 1) * lat_rows, :]) for m in range(members)
        )
        put(even_channel, jnp.where(low_lanes, one, pltpu.roll(two, 64, 1)))
        if odd_channel is not None:
            put(odd_channel, jnp.where(low_lanes, pltpu.roll(one, 64, 1), two))

    def copy_to(other):
        return pltpu.make_async_remote_copy(
            src_ref=wire_ref.at[other],
            dst_ref=got_ref.at[me],
            send_sem=send_sem.at[other],
            recv_sem=recv_sem.at[me],
            device_id={"win": other},
            device_id_type=pl.DeviceIdType.MESH,
        )

    def block_of(other):
        start = other * own_rows // PATCH
        return frame_ref[pl.ds(start, pad_rows), :].astype(jnp.bfloat16)

    low = me < windows // 2

    def deliver(slot):
        begin, count, more, extra = (
            jnp.where(low, a, b) for a, b in zip(low_plan[slot], high_plan[slot])
        )
        total = count + extra

        def owner(i):
            i = lax.rem(i + me, jnp.maximum(total, 1))
            return jnp.where(i < count, begin + i, more + i - count)

        def pack(i, carry):
            other = owner(i)
            wire_ref[other] = block_of(other)
            return carry

        def send(i, carry):
            other = owner(i)

            @pl.when(other != me)
            def _():
                copy_to(other).start()

            return carry

        lax.fori_loop(0, total, pack, 0)
        if slot == 0:
            pl.semaphore_wait(barrier, windows - 1)
        lax.fori_loop(0, total, send, 0)

    tail = CHANNELS * lat_rows
    frame_ref[tail:, :] = jnp.zeros((frame_ref.shape[0] - tail, 128), jnp.float32)
    loads[0].wait()
    for slot in range(up_tiles):
        t = jnp.where(low, up_tiles - 1 - slot, slot)
        spread(wu_ref[:, pl.ds(pl.multiple_of(t * 128, 128), 128)])
        if slot == 0:
            loads[1].wait()
            loads[2].wait()
        multiply(0, upper_levels)
        for z in range(upper_levels):
            even = t * LEVELS + 2 * z
            merge(even, even + 1 if 2 * z + 1 < LEVELS else None, z)
        if slot == 1:
            for u in range(sf_tiles):
                spread(ws_ref[:, u * 128 : (u + 1) * 128])
                multiply(upper_levels, tok_levels)
                even = VARS_UP * LEVELS + 2 * u
                merge(even, even + 1, 0)
        deliver(slot)
    got_ref[me] = block_of(me)

    tiles = image_ref.shape[1]
    lons = tiles * 128
    groups = windows // GROUP
    pitch = lons // windows
    row = lax.broadcasted_iota(jnp.int32, (128, GROUP * 128), 0)
    col = lax.broadcasted_iota(jnp.int32, (128, GROUP * 128), 1)
    target = row // 64 * 512 + (row // 4) % 4 * 128 + (row // 16) % 4 * 4 + row % 4

    def fill(i, carry):
        hit = col == target + i * pitch
        place_ref[pl.ds(pl.multiple_of(i * 128, 128), 128), :] = jnp.where(
            hit, 1.0, 0.0
        ).astype(jnp.bfloat16)
        return carry

    lax.fori_loop(0, GROUP, fill, 0)

    def arrived(source):
        pltpu.make_async_remote_copy(
            src_ref=wire_ref.at[source],
            dst_ref=got_ref.at[source],
            send_sem=send_sem.at[source],
            recv_sem=recv_sem.at[source],
            device_id={"win": source},
            device_id_type=pl.DeviceIdType.MESH,
        ).wait_recv()

    def gather(k, carry):
        g = partner(me // GROUP, k, groups)

        def wait_one(i, inner):
            source = g * GROUP + i

            @pl.when(source != me)
            def _():
                arrived(source)

            return inner

        lax.fori_loop(0, GROUP, wait_one, 0)
        stacked = jnp.concatenate([got_ref[g * GROUP + i] for i in range(GROUP)], axis=1)
        moved = jnp.dot(stacked, place_ref[...], preferred_element_type=jnp.float32)
        start = g * (GROUP * pitch) + (lons - PATCH // 2)
        shift = lax.rem(start, 128)
        tile = lax.rem(start // 128, tiles)
        after = lax.rem(tile + 1, tiles)
        first_part = lane_of_pad >= shift
        for m in range(members):
            for q in range(PATCH):
                at = (m * PATCH + q) * 128
                value = pltpu.roll(moved[:, at : at + 128], shift, 1)
                rows = pl.ds(q, pad_rows, stride=PATCH)
                image_ref[m, tile, rows, :] += jnp.where(first_part, value, 0.0)
                image_ref[m, after, rows, :] += jnp.where(first_part, 0.0, value)
        return carry

    lane_of_pad = lax.broadcasted_iota(jnp.int32, (pad_rows, 128), 1)
    image_ref[...] = jnp.zeros(image_ref.shape, jnp.float32)
    lax.fori_loop(0, groups, gather, 0)

    first_row = me * own_rows
    height = lat_rows * PATCH
    row = first_row + lax.broadcasted_iota(jnp.int32, (own_rows, 128), 0)
    first = first_row // height
    last = CHANNELS - 1
    offsets = jnp.zeros((own_rows, 128), jnp.float32)
    for i in range((own_rows - 1) // height + 2):
        channel = jnp.minimum(first + i, last)
        begins = (first + i) * height
        offsets = jnp.where(row >= begins, bias_ref[channel], offsets)
    begin = 0 if own_rows % PATCH == 0 else lax.rem(first_row, PATCH)
    for m in range(members):
        for tile in range(tiles):
            rows = image_ref[m, tile, pl.ds(begin, own_rows), :]
            out_ref[m, :, tile * 128 : (tile + 1) * 128] = (rows + offsets).astype(jnp.bfloat16)

    def sent(r, carry):
        copy_to(partner(me, r, windows)).wait_send()
        return carry

    lax.fori_loop(1, windows, sent, 0)


def write(held_ref, out_ref, sem):
    copies = [
        pltpu.make_async_copy(held_ref.at[m], out_ref.at[m], sem.at[m])
        for m in range(held_ref.shape[0])
    ]
    for copy in copies:
        copy.start()
    for copy in copies:
        copy.wait()


def plan_of(spans, lat_rows, tiles):
    owners, depth = len(spans), LEVELS * lat_rows
    surface = tiles * depth
    inner = [o for o in range(owners) if spans[o][1] <= surface]
    low, high = [], []
    done_low, done_high = inner[-1] + 1, 0
    for slot in range(tiles):
        floor = (tiles - 1 - slot) * depth
        begin = min(o for o in range(owners) if spans[o][0] >= floor)
        begin = min(begin, done_low)
        extra = owners - inner[-1] - 1 if slot == 1 else 0
        low.append((begin, done_low - begin, inner[-1] + 1, extra))
        done_low = begin
        ready = sum(1 for lo, hi in spans if hi <= (slot + 1) * depth)
        ready = owners if slot == tiles - 1 else ready
        high.append((done_high, ready - done_high, 0, 0))
        done_high = ready
    return low, high


def body(tokens, w_upper, w_surface, bias):
    members, tok_levels, lat_rows, lon_cols, width = tokens.shape
    windows = lax.axis_size("win")
    own_rows = CHANNELS * lat_rows * PATCH // windows
    lons = windows * lon_cols * PATCH
    spans = spans_of(windows, own_rows)
    pad_rows = -(-max(hi - lo for lo, hi in spans) // 16) * 16
    frame_rows = -(-(spans[-1][0] + pad_rows) // 8) * 8
    low_plan, high_plan = plan_of(spans, lat_rows, w_upper.shape[1] // 128)
    bf16, f32 = jnp.bfloat16, jnp.float32
    by_lon = jnp.transpose(tokens, (0, 1, 3, 2, 4))
    held = pl.pallas_call(
        functools.partial(kernel, (own_rows, low_plan, high_plan)),
        out_shape=jax.ShapeDtypeStruct((members, own_rows, lons), bf16),
        in_specs=[pl.BlockSpec(memory_space=pltpu.HBM)] * 3
        + [pl.BlockSpec(memory_space=pltpu.SMEM)],
        out_specs=pl.BlockSpec(memory_space=pltpu.VMEM),
        scratch_shapes=[
            pltpu.VMEM(by_lon.shape, bf16),
            pltpu.VMEM(w_upper.shape, bf16),
            pltpu.VMEM(w_surface.shape, bf16),
            pltpu.VMEM((lon_cols * width, 256), bf16),
            pltpu.VMEM((members, (tok_levels - 1) * lat_rows, 256), f32),
            pltpu.VMEM((frame_rows, 128), f32),
            pltpu.VMEM((windows, pad_rows, 128), bf16),
            pltpu.VMEM((windows, pad_rows, 128), bf16),
            pltpu.VMEM((GROUP * 128, GROUP * 128), bf16),
            pltpu.VMEM((members, lons // 128, pad_rows * PATCH, 128), f32),
            pltpu.SemaphoreType.DMA((3,)),
            pltpu.SemaphoreType.DMA((windows,)),
            pltpu.SemaphoreType.DMA((windows,)),
        ],
        compiler_params=pltpu.CompilerParams(
            collective_id=0, has_side_effects=True, vmem_limit_bytes=65 * 1000 * 1000
        ),
    )(by_lon, w_upper, w_surface, bias)
    return pl.pallas_call(
        write,
        out_shape=jax.ShapeDtypeStruct((members, own_rows, lons), bf16),
        in_specs=[pl.BlockSpec(memory_space=pltpu.VMEM)],
        out_specs=pl.BlockSpec(memory_space=pl.ANY),
        scratch_shapes=[pltpu.SemaphoreType.DMA((members,))],
    )(held)


def solution(mesh):
    placed = (P("grp", None, None, "win", None), P(), P(), P())
    return jax.shard_map(
        body, mesh=mesh, in_specs=placed, out_specs=P("grp", "win", None), check_vma=False
    )
```

```python
import functools

import jax
import jax.numpy as jnp
from jax import lax
from jax.experimental import pallas as pl
from jax.experimental.pallas import tpu as pltpu
from jax.sharding import PartitionSpec as P

VARS_UP = 5
LEVELS = 13
VARS_SF = 4
PATCH = 4
GROUP = 8
CHANNELS = VARS_UP * LEVELS + VARS_SF


def spans_of(owners, own_rows):
    return [
        (o * own_rows // PATCH, -(-(o + 1) * own_rows // PATCH)) for o in range(owners)
    ]


def selector(second, column):
    row = lax.broadcasted_iota(jnp.int32, (128, 128), 0)
    n = lax.broadcasted_iota(jnp.int32, (128, 128), 1)
    step = (n // 16) % 4 - column
    source = (n // 64) * 64 + (((n // 4) % 4 + 2 + 4 * second) % 8) * 8 + n % 4 + 4 * step
    hit = (row == source) & (step >= 0) & (step <= 1)
    return jnp.where(hit, 1.0, 0.0).astype(jnp.bfloat16)


def partner(me, r, windows):
    if windows & (windows - 1):
        return lax.rem(me + r, windows)
    return me ^ r


def kernel(
    plan, tok_hbm, wu_hbm, ws_hbm, bias_ref, out_ref,
    tok_ref, wu_ref, ws_ref, wb_ref, proj_ref, frame_ref, wire_ref, got_ref, place_ref, image_ref,
    load_sem, send_sem, recv_sem,
):
    members, tok_levels, lon_cols, lat_rows, width = tok_ref.shape
    windows, pad_rows, _ = wire_ref.shape
    upper_levels = tok_levels - 1
    up_tiles = wu_ref.shape[1] // 128
    sf_tiles = ws_ref.shape[1] // 128
    me = lax.axis_index("win")

    loads = [
        pltpu.make_async_copy(wu_hbm, wu_ref, load_sem.at[0]),
        pltpu.make_async_copy(ws_hbm, ws_ref, load_sem.at[1]),
        pltpu.make_async_copy(tok_hbm, tok_ref, load_sem.at[2]),
    ]
    for load in loads:
        load.start()

    barrier = pltpu.get_barrier_semaphore()

    def greet(r, carry):
        pl.semaphore_signal(
            barrier, inc=1, device_id={"win": partner(me, r, windows)},
            device_id_type=pl.DeviceIdType.MESH,
        )
        return carry

    lax.fori_loop(1, windows, greet, 0)

    own_rows, low_plan, high_plan = plan
    sel = jnp.concatenate(
        [selector(y, j) for j in range(lon_cols) for y in range(2)], axis=1
    )

    def spread(w):
        wide = jnp.dot(w, sel, preferred_element_type=jnp.float32).astype(jnp.bfloat16)
        for j in range(lon_cols):
            wb_ref[j * width : (j + 1) * width, :] = wide[:, j * 256 : (j + 1) * 256]

    lane = lax.broadcasted_iota(jnp.int32, (lat_rows, 128), 1)
    line = lax.broadcasted_iota(jnp.int32, (lat_rows, 128), 0)
    lower = (lane // 4) % 4 < 2
    low_lanes = lane < 64
    keep = line != jnp.where(lower, 0, lat_rows - 1)

    def image(y):
        first, second = y[:, :128], y[:, 128:]
        moved = jnp.where(
            lower, pltpu.roll(second, 1, 0), pltpu.roll(second, lat_rows - 1, 0)
        )
        return first + jnp.where(keep, moved, 0.0)

    def put(channel, block):
        start = pl.multiple_of(channel * lat_rows, 8)
        frame_ref[pl.ds(start, lat_rows), :] = block

    def multiply(z0, z1):
        rows = (z1 - z0) * lat_rows
        for m in range(members):
            total = None
            for j in range(lon_cols):
                part = jnp.dot(
                    tok_ref[m, z0:z1, j].reshape(rows, width),
                    wb_ref[j * width : (j + 1) * width, :],
                    preferred_element_type=jnp.float32,
                )
                total = part if total is None else total + part
            proj_ref[m, :rows] = total

    def merge(even_channel, odd_channel, i):
        one, two = (
            image(proj_ref[m, i * lat_rows : (i + 1) * lat_rows, :]) for m in range(members)
        )
        put(even_channel, jnp.where(low_lanes, one, pltpu.roll(two, 64, 1)))
        if odd_channel is not None:
            put(odd_channel, jnp.where(low_lanes, pltpu.roll(one, 64, 1), two))

    def copy_to(other):
        return pltpu.make_async_remote_copy(
            src_ref=wire_ref.at[other],
            dst_ref=got_ref.at[me],
            send_sem=send_sem.at[other],
            recv_sem=recv_sem.at[me],
            device_id={"win": other},
            device_id_type=pl.DeviceIdType.MESH,
        )

    def block_of(other):
        start = other * own_rows // PATCH
        return frame_ref[pl.ds(start, pad_rows), :].astype(jnp.bfloat16)

    low = me < windows // 2

    def deliver(slot):
        begin, count, more, extra = (
            jnp.where(low, a, b) for a, b in zip(low_plan[slot], high_plan[slot])
        )
        total = count + extra

        def owner(i):
            i = lax.rem(i + me, jnp.maximum(total, 1))
            return jnp.where(i < count, begin + i, more + i - count)

        def pack(i, carry):
            other = owner(i)
            wire_ref[other] = block_of(other)
            return carry

        def send(i, carry):
            other = owner(i)

            @pl.when(other != me)
            def _():
                copy_to(other).start()

            return carry

        lax.fori_loop(0, total, pack, 0)
        if slot == 0:
            pl.semaphore_wait(barrier, windows - 1)
        lax.fori_loop(0, total, send, 0)

    tail = CHANNELS * lat_rows
    frame_ref[tail:, :] = jnp.zeros((frame_ref.shape[0] - tail, 128), jnp.float32)
    loads[0].wait()
    for slot in range(up_tiles):
        t = jnp.where(low, up_tiles - 1 - slot, slot)
        spread(wu_ref[:, pl.ds(pl.multiple_of(t * 128, 128), 128)])
        if slot == 0:
            loads[1].wait()
            loads[2].wait()
        multiply(0, upper_levels)
        for z in range(upper_levels):
            even = t * LEVELS + 2 * z
            merge(even, even + 1 if 2 * z + 1 < LEVELS else None, z)
        if slot == 1:
            for u in range(sf_tiles):
                spread(ws_ref[:, u * 128 : (u + 1) * 128])
                multiply(upper_levels, tok_levels)
                even = VARS_UP * LEVELS + 2 * u
                merge(even, even + 1, 0)
        deliver(slot)
    got_ref[me] = block_of(me)

    tiles = image_ref.shape[1]
    lons = tiles * 128
    groups = windows // GROUP
    pitch = lons // windows
    row = lax.broadcasted_iota(jnp.int32, (128, GROUP * 128), 0)
    col = lax.broadcasted_iota(jnp.int32, (128, GROUP * 128), 1)
    target = row // 64 * 512 + (row // 4) % 4 * 128 + (row // 16) % 4 * 4 + row % 4

    def fill(i, carry):
        hit = col == target + i * pitch
        place_ref[pl.ds(pl.multiple_of(i * 128, 128), 128), :] = jnp.where(
            hit, 1.0, 0.0
        ).astype(jnp.bfloat16)
        return carry

    lax.fori_loop(0, GROUP, fill, 0)

    def arrived(source):
        pltpu.make_async_remote_copy(
            src_ref=wire_ref.at[source],
            dst_ref=got_ref.at[source],
            send_sem=send_sem.at[source],
            recv_sem=recv_sem.at[source],
            device_id={"win": source},
            device_id_type=pl.DeviceIdType.MESH,
        ).wait_recv()

    def gather(k, carry):
        g = partner(me // GROUP, k, groups)

        def wait_one(i, inner):
            source = g * GROUP + i

            @pl.when(source != me)
            def _():
                arrived(source)

            return inner

        lax.fori_loop(0, GROUP, wait_one, 0)
        stacked = jnp.concatenate([got_ref[g * GROUP + i] for i in range(GROUP)], axis=1)
        moved = jnp.dot(stacked, place_ref[...], preferred_element_type=jnp.float32)
        start = g * (GROUP * pitch) + (lons - PATCH // 2)
        shift = lax.rem(start, 128)
        tile = lax.rem(start // 128, tiles)
        after = lax.rem(tile + 1, tiles)
        first_part = lane_of_pad >= shift
        for m in range(members):
            for q in range(PATCH):
                at = (m * PATCH + q) * 128
                value = pltpu.roll(moved[:, at : at + 128], shift, 1)
                rows = pl.ds(q, pad_rows, stride=PATCH)
                image_ref[m, tile, rows, :] += jnp.where(first_part, value, 0.0)
                image_ref[m, after, rows, :] += jnp.where(first_part, 0.0, value)
        return carry

    lane_of_pad = lax.broadcasted_iota(jnp.int32, (pad_rows, 128), 1)
    image_ref[...] = jnp.zeros(image_ref.shape, jnp.float32)
    lax.fori_loop(0, groups, gather, 0)

    first_row = me * own_rows
    height = lat_rows * PATCH
    row = first_row + lax.broadcasted_iota(jnp.int32, (own_rows, 128), 0)
    first = first_row // height
    last = CHANNELS - 1
    offsets = jnp.zeros((own_rows, 128), jnp.float32)
    for i in range((own_rows - 1) // height + 2):
        channel = jnp.minimum(first + i, last)
        begins = (first + i) * height
        offsets = jnp.where(row >= begins, bias_ref[channel], offsets)
    begin = 0 if own_rows % PATCH == 0 else lax.rem(first_row, PATCH)
    for m in range(members):
        for tile in range(tiles):
            rows = image_ref[m, tile, pl.ds(begin, own_rows), :]
            out_ref[m, :, tile * 128 : (tile + 1) * 128] = (rows + offsets).astype(jnp.bfloat16)

    def sent(r, carry):
        copy_to(partner(me, r, windows)).wait_send()
        return carry

    lax.fori_loop(1, windows, sent, 0)


def write(held_hbm, out_hbm, part_ref, sem):
    members, cuts, _, lanes = part_ref.shape
    pieces = [(m, i) for m in range(members) for i in range(cuts)]

    def view(ref, m, i):
        return ref.at[m, :, i * lanes : (i + 1) * lanes]

    reads = [
        pltpu.make_async_copy(view(held_hbm, m, i), part_ref.at[m, i], sem.at[0, m, i])
        for m, i in pieces
    ]
    writes = [
        pltpu.make_async_copy(part_ref.at[m, i], view(out_hbm, m, i), sem.at[1, m, i])
        for m, i in pieces
    ]
    for read in reads:
        read.start()
    for read, copy in zip(reads, writes):
        read.wait()
        copy.start()
    for copy in writes:
        copy.wait()


def plan_of(spans, lat_rows, tiles):
    owners, depth = len(spans), LEVELS * lat_rows
    surface = tiles * depth
    inner = [o for o in range(owners) if spans[o][1] <= surface]
    low, high = [], []
    done_low, done_high = inner[-1] + 1, 0
    for slot in range(tiles):
        floor = (tiles - 1 - slot) * depth
        begin = min(o for o in range(owners) if spans[o][0] >= floor)
        begin = min(begin, done_low)
        extra = owners - inner[-1] - 1 if slot == 1 else 0
        low.append((begin, done_low - begin, inner[-1] + 1, extra))
        done_low = begin
        ready = sum(1 for lo, hi in spans if hi <= (slot + 1) * depth)
        ready = owners if slot == tiles - 1 else ready
        high.append((done_high, ready - done_high, 0, 0))
        done_high = ready
    return low, high


def body(tokens, w_upper, w_surface, bias):
    members, tok_levels, lat_rows, lon_cols, width = tokens.shape
    windows = lax.axis_size("win")
    own_rows = CHANNELS * lat_rows * PATCH // windows
    lons = windows * lon_cols * PATCH
    spans = spans_of(windows, own_rows)
    pad_rows = -(-max(hi - lo for lo, hi in spans) // 16) * 16
    frame_rows = -(-(spans[-1][0] + pad_rows) // 8) * 8
    low_plan, high_plan = plan_of(spans, lat_rows, w_upper.shape[1] // 128)
    bf16, f32 = jnp.bfloat16, jnp.float32
    by_lon = jnp.transpose(tokens, (0, 1, 3, 2, 4))
    held = pl.pallas_call(
        functools.partial(kernel, (own_rows, low_plan, high_plan)),
        out_shape=jax.ShapeDtypeStruct((members, own_rows, lons), bf16),
        in_specs=[pl.BlockSpec(memory_space=pltpu.HBM)] * 3
        + [pl.BlockSpec(memory_space=pltpu.SMEM)],
        out_specs=pl.BlockSpec(memory_space=pltpu.VMEM),
        scratch_shapes=[
            pltpu.VMEM(by_lon.shape, bf16),
            pltpu.VMEM(w_upper.shape, bf16),
            pltpu.VMEM(w_surface.shape, bf16),
            pltpu.VMEM((lon_cols * width, 256), bf16),
            pltpu.VMEM((members, (tok_levels - 1) * lat_rows, 256), f32),
            pltpu.VMEM((frame_rows, 128), f32),
            pltpu.VMEM((windows, pad_rows, 128), bf16),
            pltpu.VMEM((windows, pad_rows, 128), bf16),
            pltpu.VMEM((GROUP * 128, GROUP * 128), bf16),
            pltpu.VMEM((members, lons // 128, pad_rows * PATCH, 128), f32),
            pltpu.SemaphoreType.DMA((3,)),
            pltpu.SemaphoreType.DMA((windows,)),
            pltpu.SemaphoreType.DMA((windows,)),
        ],
        compiler_params=pltpu.CompilerParams(
            collective_id=0, has_side_effects=True, vmem_limit_bytes=65 * 1000 * 1000
        ),
    )(by_lon, w_upper, w_surface, bias)
    return pl.pallas_call(
        write,
        out_shape=jax.ShapeDtypeStruct((members, own_rows, lons), bf16),
        in_specs=[pl.BlockSpec(memory_space=pl.ANY)],
        out_specs=pl.BlockSpec(memory_space=pl.ANY),
        scratch_shapes=[
            pltpu.VMEM((members, 3, own_rows, lons // 3), bf16),
            pltpu.SemaphoreType.DMA((2, members, 3)),
        ],
    )(held)


def solution(mesh):
    placed = (P("grp", None, None, "win", None), P(), P(), P())
    return jax.shard_map(
        body, mesh=mesh, in_specs=placed, out_specs=P("grp", "win", None), check_vma=False
    )
```
